128 devices in a mesh: dev: 32 (over y, x, core), ka: 4 (over z).
Axes of the slice: x: 4, y: 4, z: 4, core: 2. Of those that a mesh axis runs over, the one named last changes fastest.
Arguments:
- tile_data: float32 [8192, 128, 128], P(('dev', 'ka')), may hold values from -0.25 to 0.25
- tile_row: int32 [128, 64], P(('dev', 'ka')), may hold values from 0 to 31
- tile_col: int32 [128, 64], P(('dev', 'ka')), may hold values from 0 to 63
- tile_count: int32 [128], P(('dev', 'ka')), may hold values from 10 to 64, as said below
- touched: int32 [128, 64], P(('dev', 'ka')), may hold values from 0 to 511, as said below
- owner_map: int32 [512], replicated, may hold values from 0 to 511, as said below
- observed: float32 [4096, 128, 64], P(('dev', 'ka')), may hold values from -6 to 6
- start_x: float32 [8192, 128, 64], P(('dev', 'ka')), may hold values from -6 to 6
- start_u: float32 [8192, 128, 64], P(('dev', 'ka')), may hold values from -4 to 4
Outputs:
- final_x: float32 [8192, 128, 64], P(('dev', 'ka'))
- final_u: float32 [8192, 128, 64], P(('dev', 'ka'))
- z_keeper_agreed: float32 [512, 128, 64], P(('dev', 'ka'))
- primal_gap: float32 [64], replicated
The draws below stay inside these ranges and needn't reach their ends.
Inputs may be any that keep to these rules, and one draw needn't show every extreme that they name: Shard s uses its first tile_count[s] slots; each count is at least 10 and at most 64, and some shard has exactly 64. `touched`: A shard's 64 entries are distinct column blocks. The owner of block j is shard owner_map[j] // 4; a shard touches at most one block of any one owner, and every shard touches exactly one block of some owner. `owner_map`: A permutation of 0 to 511.
All inputs are finite; a program needn't handle non-finite values.
Results may differ from the reference program's by a relative error of at most 0.0003.
Values sent between devices are 32-bit elements.
A program may use at most 128 MiB of HBM per device.

```python
import math
import jax
import jax.numpy as jnp
import numpy as np
from jax import lax

BLK = 128
TARGETS = 64
TILE_DEV = 64
ROWB_DEV = 32
LOCAL_COLS = 64
COL_DEV = 4
ITERS = 2
CG_STEPS = 4
PIECE_TOTAL = 128
OWNER_LIMIT = 1
COLB = 512
TILES = 8192
ROWBLOCKS = 4096
SLOTS = 8192


def column_plan(key):
    ordering = jax.random.permutation(jax.random.fold_in(key, 11), COLB).astype(jnp.int32)
    inverse = jnp.zeros((COLB,), jnp.int32).at[ordering].set(jnp.arange(COLB, dtype=jnp.int32))
    keeper_demand = jax.random.randint(jax.random.fold_in(key, 12), (PIECE_TOTAL,), 0, 8, dtype=jnp.int32)
    block_heat = jax.random.randint(jax.random.fold_in(key, 13), (PIECE_TOTAL, COL_DEV), 0, 8, dtype=jnp.int32)
    local_noise = jax.random.randint(jax.random.fold_in(key, 14), (PIECE_TOTAL, PIECE_TOTAL, COL_DEV), 0, 1024, dtype=jnp.int32)
    local_score = local_noise * (1 + block_heat * block_heat)[None, :, :] * COL_DEV + jnp.arange(COL_DEV, dtype=jnp.int32)
    local_pick = lax.top_k(local_score, OWNER_LIMIT)[1].astype(jnp.int32)
    couple_jitter = jax.random.randint(jax.random.fold_in(key, 15), (PIECE_TOTAL, PIECE_TOTAL, OWNER_LIMIT), 0, 1024, dtype=jnp.int32)
    preferred_keeper = jax.random.randint(jax.random.fold_in(key, 16), (PIECE_TOTAL,), 0, PIECE_TOTAL, dtype=jnp.int32)
    preference_reward = (jnp.arange(PIECE_TOTAL, dtype=jnp.int32)[None, :] == preferred_keeper[:, None]).astype(jnp.int32) * (1 << 28)
    couple_position = jnp.arange(PIECE_TOTAL * OWNER_LIMIT, dtype=jnp.int32).reshape(PIECE_TOTAL, OWNER_LIMIT)
    couple_rating = couple_jitter * (1 + keeper_demand * keeper_demand)[None, :, None] * (PIECE_TOTAL * OWNER_LIMIT) + couple_position[None, :, :] + preference_reward[:, :, None]
    chosen = lax.top_k(couple_rating.reshape(PIECE_TOTAL, PIECE_TOTAL * OWNER_LIMIT), LOCAL_COLS)[1].astype(jnp.int32)
    owners = chosen // OWNER_LIMIT
    local_ids = jnp.take_along_axis(local_pick.reshape(PIECE_TOTAL, PIECE_TOTAL * OWNER_LIMIT), chosen, axis=1)
    touched_ids = inverse[owners * COL_DEV + local_ids]
    return (ordering, touched_ids.astype(jnp.int32))


def draw_touched(key, part):
    return column_plan(key)[1]


def draw_owner_map(key, part):
    return column_plan(key)[0]


def draw_tile_count(key, part):
    levels = jax.random.randint(jax.random.fold_in(key, 3), (PIECE_TOTAL,), 0, 6, dtype=jnp.int32)
    counts = TILE_DEV // (1 + levels)
    busiest = jax.random.randint(jax.random.fold_in(key, 4), (), 0, PIECE_TOTAL, dtype=jnp.int32)
    return jnp.where(jnp.arange(PIECE_TOTAL, dtype=jnp.int32) == busiest, TILE_DEV, counts).astype(jnp.int32)


def touch_ends(drawn, key, least, largest):
    longest = drawn.shape.index(max(drawn.shape))
    spots = []
    for shift in (0, 1):
        where = [jax.random.randint(jax.random.fold_in(key, axis), (), 0, length) for axis, length in enumerate(drawn.shape)]
        where[longest] = (where[longest] + shift) % drawn.shape[longest]
        spots.append(tuple(where))
    return drawn.at[spots[0]].set(least).at[spots[1]].set(largest)


def block_levels(key, extent, pieces, low, top_value):
    factor_of = 1.0
    for position, shards_of in pieces:
        steps = jax.random.uniform(jax.random.fold_in(jax.random.fold_in(key, 6), position), (shards_of,), jnp.float32, low / len(pieces), top_value / len(pieces))
        factor_of = factor_of * jnp.repeat(jnp.exp(steps), extent[position] // shards_of).reshape((-1,) + (1,) * (len(extent) - 1 - position))
    return factor_of


def cumulative_ranks(number_of, lean):
    loads = [(1 << 20) // math.isqrt(standing ** lean) + 1 for standing in range(1, number_of + 1)]
    width = 1 + sum(loads) // (1 << 30)
    return np.cumsum(np.array([max(1, weight // width) for weight in loads]))


def ranked(own_key, shape, count, slope):
    table = cumulative_ranks(count, slope)
    lot = jax.random.randint(jax.random.fold_in(own_key, 1), shape, 0, int(table[count - 1]))
    rank = jnp.searchsorted(jnp.asarray(table, jnp.int32), lot, side="right")
    return jax.random.permutation(jax.random.fold_in(own_key, 2), count)[rank].astype(jnp.int32)


def normal_values(own_key, shape, scale, most, split=(), kind=jnp.bfloat16):
    level = block_levels(own_key, shape, split, -0.22, 0.18) if split else 1.0
    drawn = jax.random.normal(own_key, shape, jnp.float32) * scale * level
    return jnp.minimum(jnp.maximum(drawn, -most), most).astype(kind)


def setup_inputs(seed: int = 0) -> dict:
    splits = jax.random.split(jax.random.key(seed), 10)
    tile_data = normal_values(splits[0], (TILES, BLK, BLK), (4 * BLK) ** -0.5, 0.25, ((0, 128),), jnp.float32)
    tile_row = touch_ends(jax.random.randint(splits[1], (PIECE_TOTAL, TILE_DEV), 0, ROWB_DEV), jax.random.fold_in(splits[1], 1), 0, ROWB_DEV - 1).astype(jnp.int32)
    tile_col = touch_ends(ranked(splits[2], (PIECE_TOTAL, TILE_DEV), LOCAL_COLS, 2), jax.random.fold_in(splits[2], 3), 0, LOCAL_COLS - 1).astype(jnp.int32)
    tile_count = draw_tile_count(jax.random.fold_in(splits[9], 71), 0)
    touched = draw_touched(jax.random.fold_in(splits[9], 71), 0)
    owner_map = draw_owner_map(jax.random.fold_in(splits[9], 71), 0)
    observed = normal_values(splits[6], (ROWBLOCKS, BLK, TARGETS), 1.0, 6.0, ((0, 128),), jnp.float32)
    start_x = normal_values(splits[7], (SLOTS, BLK, TARGETS), 1.0, 6.0, ((0, 128),), jnp.float32)
    start_u = normal_values(splits[8], (SLOTS, BLK, TARGETS), 0.5, 4.0, ((0, 128),), jnp.float32)
    return dict(tile_data=tile_data, tile_row=tile_row, tile_col=tile_col, tile_count=tile_count, touched=touched, owner_map=owner_map, observed=observed, start_x=start_x, start_u=start_u)


EXACTNESS = lax.Precision.HIGHEST
PENALTY = 1.0
COUPLING = 1.0

def shrink(amount, cutoff):
    return amount - jnp.clip(amount, -cutoff, cutoff)

def forward(tile_set, row_ids, col_ids, in_use, vector):
    product = jnp.einsum('tij,tjr->tir', tile_set, vector[col_ids], precision=EXACTNESS) * in_use[:, None, None]
    return jax.ops.segment_sum(product, row_ids, ROWB_DEV)

def backward(tile_set, row_ids, col_ids, in_use, vector):
    product = jnp.einsum('tji,tjr->tir', tile_set, vector[row_ids], precision=EXACTNESS) * in_use[:, None, None]
    return jax.ops.segment_sum(product, col_ids, LOCAL_COLS)

def pull_one(packed):
    tile_set, row_ids, col_ids, in_use, observed_set = packed
    return backward(tile_set, row_ids, col_ids, in_use, observed_set)

def conjugate(packed):
    tile_set, row_ids, col_ids, in_use, rhs_side, begin = packed

    def operate(vector):
        image_rows = forward(tile_set, row_ids, col_ids, in_use, vector)
        return backward(tile_set, row_ids, col_ids, in_use, image_rows) + COUPLING * vector
    iterate = begin
    residual = rhs_side - operate(begin)
    direction = residual
    norm_now = lax.optimization_barrier(jnp.sum(residual * residual, axis=(0, 1)))
    for cg_step in range(CG_STEPS):
        mapped = operate(direction)
        step_size = norm_now / lax.optimization_barrier(jnp.sum(direction * mapped, axis=(0, 1)))
        iterate = iterate + step_size * direction
        residual = residual - step_size * mapped
        norm_next = lax.optimization_barrier(jnp.sum(residual * residual, axis=(0, 1)))
        direction = residual + norm_next / norm_now * direction
        norm_now = norm_next
    return iterate

def reference(tile_data, tile_row, tile_col, tile_count, touched, owner_map, observed, start_x, start_u):
    tile_sets = tile_data.reshape(PIECE_TOTAL, TILE_DEV, BLK, BLK)
    observed_sets = observed.reshape(PIECE_TOTAL, ROWB_DEV, BLK, TARGETS)
    current_x = start_x.reshape(PIECE_TOTAL, LOCAL_COLS, BLK, TARGETS)
    current_u = start_u.reshape(PIECE_TOTAL, LOCAL_COLS, BLK, TARGETS)
    in_use = (jnp.arange(TILE_DEV, dtype=jnp.int32)[None, :] < tile_count[:, None]).astype(jnp.float32)
    pulled = lax.map(pull_one, (tile_sets, tile_row, tile_col, in_use, observed_sets))
    flat_ids = touched.reshape(-1)
    counts = jax.ops.segment_sum(jnp.ones(flat_ids.shape, jnp.float32), flat_ids, COLB)
    share = jnp.maximum(counts, 1.0)[:, None, None]
    consensus = jnp.zeros((COLB, BLK, TARGETS), jnp.float32)
    difference = jnp.zeros_like(current_x)
    for outer_step in range(ITERS):
        merged = (current_x + current_u).reshape(SLOTS, BLK, TARGETS)
        summed = jax.ops.segment_sum(merged, flat_ids, COLB)
        consensus = shrink(summed / share, PENALTY / (COUPLING * share))
        z_local = consensus[touched]
        difference = current_x - z_local
        current_u = current_u + difference
        rhs_side = pulled + COUPLING * (z_local - current_u)
        current_x = lax.map(conjugate, (tile_sets, tile_row, tile_col, in_use, rhs_side, current_x))
    primal_gap = jnp.sqrt(lax.optimization_barrier(jnp.sum(difference * difference, axis=(0, 1, 2))) / (PIECE_TOTAL * LOCAL_COLS * BLK))
    z_keeper_agreed = jnp.zeros_like(consensus).at[owner_map].set(consensus)
    return (current_x.reshape(SLOTS, BLK, TARGETS), current_u.reshape(SLOTS, BLK, TARGETS), z_keeper_agreed, primal_gap)
```

```python
import functools

import jax
import jax.numpy as jnp
from jax import lax
from jax.experimental import pallas as pl
from jax.experimental.pallas import tpu as pltpu
from jax.sharding import PartitionSpec as P

ITERS = 2
CG_STEPS = 4
PENALTY = 1.0
COUPLING = 1.0
AXES = ("dev", "ka")
MESH = pl.DeviceIdType.MESH
MIB = 1 << 20
VMEM_MIB = 61
PIECE = 8
ORDERS = ("zyx", "yxz", "xzy")
SLOT, MAIL, FWD_TILE, FWD_FROM, FWD_FIRST, BWD_TILE, BWD_FROM, BWD_FIRST, ROW_LAST, COL_LAST = (
    0, 3, 6, 7, 8, 9, 10, 11, 12, 13,
)


def split(value):
    high = value.astype(jnp.bfloat16)
    low = (value - high.astype(jnp.float32)).astype(jnp.bfloat16)
    return jnp.concatenate([high, low], axis=0)


def lanes(total):
    return jnp.sum(total, axis=1, keepdims=True)


def kernel(
    n, cb, mean_of,
    tab, tags_ref, tile_hbm, obs_hbm, x_hbm, u_hbm,
    x_ref, u_ref, zown_ref, gap_ref,
    tile_ref, obs_ref, fwd_ref, bwd_ref, pb_ref, wb_ref, wseg, qseg, r_ref, p_ref, zu_ref,
    box, in1, sum1, in2, sum2, in3, zz2, zz1, ans, zbox, tagin, tagx, share_ref, gin,
    load_sem, r1_s, r1_r, r2_s, r2_r, r3_s, r3_r, b3_s, b3_r, b2_s, b2_r, b1_s, b1_r,
    tag_s, tag_r, gap_s, gap_r,
):
    slots, blk, _ = tile_ref.shape
    local_cols, targets, _ = x_ref.shape
    row_blocks = obs_ref.shape[0]
    subs = targets // PIECE
    plane = n * n
    groups = 2 * n
    f32 = jnp.float32
    md, mk = lax.axis_index(AXES[0]), lax.axis_index(AXES[1])
    at = {"c": lax.rem(md, 2), "x": lax.rem(md // 2, n), "y": md // (2 * n), "z": mk}

    def device(axis, da, dc=0):
        place = dict(at)
        place[axis] = lax.rem(place[axis] + da, n)
        place["c"] = lax.rem(place["c"] + dc, 2)
        return ((place["y"] * n + place["x"]) * 2 + place["c"], place["z"])

    def remote(source, target, send_sem, recv_sem, where):
        return pltpu.make_async_remote_copy(
            source, target, send_sem, recv_sem, device_id=where, device_id_type=MESH
        )

    def order(k):
        return k % 3 if k < subs else 0

    def axis(k, level):
        return ORDERS[order(k)][level]

    def back(da):
        return (n - da) % n

    line = [(dc, da) for dc in range(2) for da in range(n)][1:]
    anyone = device("x", 1)

    def line_sends(k, p, source, target, send_sem, recv_sem):
        for dc, da in line:
            mine, theirs = (dc * n + da) * plane, (dc * n + back(da)) * plane
            remote(
                source.at[k, pl.ds(mine, plane)], target.at[k, pl.ds(theirs, plane)],
                send_sem.at[k], recv_sem.at[k], device(ORDERS[p][0], da, dc),
            ).start()

    def ring_sends(k, where, pick, size, source, target, send_sem, recv_sem):
        for da in range(1, n):
            remote(
                source.at[k, pl.ds(da * size if pick else 0, size)],
                target.at[k, pl.ds(back(da) * size, size)],
                send_sem.at[k], recv_sem.at[k], device(where, da),
            ).start()

    def rest(ref, k, size):
        return ref.at[k, pl.ds(size, ref.shape[1] - size)]

    def arrived(ref, k, size, sems):
        part = rest(ref, k, size)
        remote(part, part, sems[0].at[k], sems[1].at[k], anyone).wait_recv()

    def left(ref, k, size, sems):
        part = rest(ref, k, size)
        remote(part, part, sems[0].at[k], sems[1].at[k], anyone).wait_send()

    r1, r2, r3 = (r1_s, r1_r), (r2_s, r2_r), (r3_s, r3_r)
    b3, b2, b1 = (b3_s, b3_r), (b2_s, b2_r), (b1_s, b1_r)
    tagged = (tag_s, tag_r)

    greeted = [device(ORDERS[0][0], da, dc) for dc, da in line]
    for where in ORDERS[0][1:]:
        greeted += [device(where, da, dc) for dc in range(2) for da in range(1, n)]
    barrier = pltpu.get_barrier_semaphore()
    for where in greeted:
        pl.semaphore_signal(barrier, inc=1, device_id=where, device_id_type=MESH)

    loads = [
        pltpu.make_async_copy(source, target, load_sem.at[i])
        for i, (source, target) in enumerate(
            ((x_hbm, x_ref), (u_hbm, u_ref), (tile_hbm, tile_ref), (obs_hbm, obs_ref))
        )
    ]
    for one in loads:
        one.start()

    def members(p):
        return [k for k in range(subs) if order(k) == p]

    def build(p):
        def one(i, carry):
            for g in range(groups):
                q = g * plane + i
                slot = tab[SLOT + p, q]
                for k in members(p):
                    rows = pl.ds(k * PIECE, PIECE)
                    box[k, q] = x_ref[slot, rows] + u_ref[slot, rows]
            return carry

        lax.fori_loop(0, plane, one, 0)

    def send_r1(k):
        line_sends(k, order(k), box, in1, *r1)

    def send_r2(k):
        ring_sends(k, axis(k, 1), True, n * cb, sum1, in2, *r2)

    def t1(k):
        p = order(k)
        arrived(in1, k, plane, r1)

        def one(i, carry):
            total = [jnp.zeros((PIECE, blk), f32)] * cb
            for s in range(groups):
                value = box[k, i] if s == 0 else in1[k, s * plane + i]
                tag = tagx[p, i * groups + s]
                total = [t + jnp.where(tag == b, value, 0.0) for b, t in enumerate(total)]
            for b in range(cb):
                sum1[k, i * cb + b] = total[b]
            return carry

        lax.fori_loop(0, plane, one, 0, unroll=2)
        send_r2(k)

    def t2(k):
        size = n * cb
        arrived(in2, k, size, r2)
        for j in range(size):
            total = sum1[k, j]
            for s in range(1, n):
                total = total + in2[k, s * size + j]
            sum2[k, j] = total
        ring_sends(k, axis(k, 2), True, cb, sum2, in3, *r3)

    def total3(k, b):
        total = sum2[k, b]
        for s in range(1, n):
            total = total + in3[k, s * cb + b]
        return total

    def t3(k):
        arrived(in3, k, cb, r3)
        for b in range(cb):
            share = share_ref[b]
            amount = total3(k, b) / share
            cutoff = PENALTY / (COUPLING * share)
            z = amount - jnp.clip(amount, -cutoff, cutoff)
            zz2[k, b] = z
            zown_ref[b, pl.ds(k * PIECE, PIECE)] = z
        ring_sends(k, axis(k, 2), False, cb, zz2, zz2, *b3)

    def t4(k):
        arrived(zz2, k, cb, b3)
        for j in range(n * cb):
            zz1[k, j] = zz2[k, j]
        ring_sends(k, axis(k, 1), False, n * cb, zz2, zz1, *b2)

    def t5(k):
        p = order(k)
        arrived(zz1, k, n * cb, b2)

        def one(i, carry):
            z = [zz1[k, i * cb + b] for b in range(cb)]
            for s in range(groups):
                tag = tagx[p, i * groups + s]
                value = z[cb - 1]
                for b in range(cb - 1):
                    value = jnp.where(tag == b, z[b], value)
                if s == 0:
                    zbox[k, i] = value
                else:
                    ans[k, s * plane + i] = value
            return carry

        lax.fori_loop(0, plane, one, 0, unroll=2)
        line_sends(k, p, ans, zbox, *b1)

    waves = [list(range(f, min(f + 3, subs))) for f in range(0, subs, 3)]

    def start_exchange():
        for p in range(3):
            build(p)

    def exchange(first):
        last = len(waves) - 1
        if first:
            t2(subs)
        for tick in range(2 * last + 5):
            for level, task in ((5, t5), (4, t4), (3, t3), (2, t2), (1, t1)):
                late = tick - (level - 1)
                if late < 0 or late % 2:
                    continue
                w = late // 2
                if w > last:
                    continue
                for k in waves[w]:
                    task(k)
                    if level == 1 and k + 6 < subs:
                        send_r1(k + 6)
            if first and tick == 0:
                arrived(in3, subs, cb, r3)
                for b in range(cb):
                    share_ref[b] = jnp.maximum(total3(subs, b), 1.0)
        for k in range(subs):
            arrived(zbox, k, plane, b1)
        for k in range(subs + 1 if first else subs):
            left(sum1, k, n * cb, r2)
            left(sum2, k, cb, r3)
        for k in range(subs):
            left(box, k, plane, r1)
            left(in3, k, cb, b3)
            left(zz1, k, n * cb, b2)
            left(ans, k, plane, b1)

    def tile_pass(tiles_ref, from_row, first_row, source_ref, seg_ref):
        group = min(16, slots)

        def step(number, total):
            for inner in range(group):
                t = number * group + inner
                lhs = source_ref[tab[from_row, t]]
                out = jnp.dot(
                    jnp.concatenate([lhs, lhs], axis=1), tiles_ref[t],
                    preferred_element_type=f32,
                )
                fresh = tab[first_row, t] == 1
                total = jnp.where(fresh, 0.0, total) + (out[:targets] + out[targets:])
                seg_ref[t] = total
            return total

        lax.fori_loop(0, slots // group, step, jnp.zeros((targets, blk), f32))

    def forward():
        tile_pass(fwd_ref, FWD_FROM, FWD_FIRST, pb_ref, wseg)

    def backward():
        tile_pass(bwd_ref, BWD_FROM, BWD_FIRST, wb_ref, qseg)

    def loop(count, body, init=0, unroll=4):
        return lax.fori_loop(0, count, body, init, unroll=unroll)

    zero = jnp.zeros((targets, blk), f32)
    wseg[slots] = zero
    qseg[slots] = zero

    loads[0].wait()
    loads[1].wait()
    start_exchange()
    pl.semaphore_wait(barrier, len(greeted))
    for p in range(3):
        line_sends(p, p, tags_ref, tagin, *tagged)
    for k in range(min(6, subs)):
        send_r1(k)

    def opening(c, carry):
        pb_ref[c] = split(x_ref[c])
        return carry

    loop(local_cols, opening)
    loads[2].wait()

    def convert(t, carry):
        fwd_ref[t] = split(tile_ref[tab[FWD_TILE, t]].T)
        bwd_ref[t] = split(tile_ref[tab[BWD_TILE, t]])
        return carry

    loop(slots, convert)

    for p in range(3):
        arrived(tagin, p, plane, tagged)
        left(tagin, p, plane, tagged)

        def expand(i, carry):
            for s in range(groups):
                q = s * plane + i
                row = (tags_ref if s == 0 else tagin)[p, pl.ds(q, 1)]
                tagx[p, i * groups + s] = jnp.broadcast_to(row, (PIECE, blk))
            return carry

        loop(plane, expand, unroll=1)

    def census(i, carry):
        total = [jnp.zeros((PIECE, blk), f32)] * cb
        for s in range(groups):
            tag = tagx[0, i * groups + s]
            total = [t + jnp.where(tag == b, 1.0, 0.0) for b, t in enumerate(total)]
        for b in range(cb):
            sum1[subs, i * cb + b] = total[b]
        return carry

    loop(plane, census, unroll=1)
    send_r2(subs)

    forward()
    loads[3].wait()

    def against(r, carry):
        wb_ref[r] = split(obs_ref[r] - wseg[tab[ROW_LAST, r]])
        return carry

    loop(row_blocks, against)
    backward()

    def basis(c, carry):
        r_ref[c] = qseg[tab[COL_LAST, c]] - COUPLING * x_ref[c]
        return carry

    loop(local_cols, basis)
    exchange(True)

    gap_line = ORDERS[0]

    def gap_send(stage):
        if stage == 0:
            for dc, da in line:
                remote(
                    gin.at[0, pl.ds(0, 1)], gin.at[0, pl.ds(dc * n + back(da), 1)],
                    gap_s.at[0], gap_r.at[0], device(gap_line[0], da, dc),
                ).start()
        else:
            ring_sends(stage, gap_line[stage], False, 1, gin, gin, gap_s, gap_r)

    def gap_total(stage):
        count = groups if stage == 0 else n
        part = gin.at[stage, pl.ds(1, count - 1)]
        one = remote(part, part, gap_s.at[stage], gap_r.at[stage], anyone)
        one.wait_recv()
        one.wait_send()
        total = gin[stage, 0]
        for s in range(1, count):
            total = total + gin[stage, s]
        return total

    for outer_step in range(ITERS):
        last = outer_step == ITERS - 1

        def begin(c, carry):
            rr, gap = carry
            z = jnp.concatenate(
                [zbox[k, tab[MAIL + order(k), c]] for k in range(subs)], axis=0
            )
            d = x_ref[c] - z
            u = u_ref[c] + d
            u_ref[c] = u
            zu = z - u
            r = r_ref[c] + COUPLING * zu
            r_ref[c] = r
            p_ref[c] = r
            pb_ref[c] = split(r)
            if last:
                gap = gap + d * d
            else:
                zu_ref[c] = zu
            return rr + r * r, gap

        rr, gap = loop(local_cols, begin, (zero, zero), unroll=2)
        rr = lanes(rr)
        pp = rr
        if last:
            gin[0, 0] = lax.dot_general(
                jnp.ones((PIECE, blk), f32),
                jnp.concatenate([gap, jnp.zeros((blk - targets, blk), f32)], axis=0),
                (((1,), (1,)), ((), ())),
                precision=lax.Precision.HIGHEST, preferred_element_type=f32,
            )
            gap_send(0)

        for step in range(CG_STEPS):
            closing = step == CG_STEPS - 1
            forward()

            def image(i, ww):
                w = wseg[tab[ROW_LAST, i]]
                if not (last and closing):
                    wb_ref[i] = split(w)
                return ww + w * w

            ww = lanes(loop(row_blocks, image, zero))
            size = rr / (ww + COUPLING * pp)
            if closing:

                def finish(c, carry):
                    x_ref[c] = x_ref[c] + size * p_ref[c]
                    return carry

                loop(local_cols, finish)
                if last:
                    break
                start_exchange()
                for k in range(min(6, subs)):
                    send_r1(k)
                backward()

                def close(c, carry):
                    q = qseg[tab[COL_LAST, c]] + COUPLING * p_ref[c]
                    r_ref[c] = r_ref[c] - size * q - COUPLING * zu_ref[c]
                    return carry

                loop(local_cols, close)
                exchange(False)
                break
            backward()
            if last and step < 2:
                gin[step + 1, 0] = gap_total(step)
                gap_send(step + 1)

            def reduce(c, total):
                q = qseg[tab[COL_LAST, c]] + COUPLING * p_ref[c]
                r = r_ref[c] - size * q
                r_ref[c] = r
                return total + r * r

            norm = lanes(loop(local_cols, reduce, zero))
            turn = norm / rr

            def direct(c, total):
                old = p_ref[c]
                x_ref[c] = x_ref[c] + size * old
                p = r_ref[c] + turn * old
                p_ref[c] = p
                pb_ref[c] = split(p)
                return total + p * p

            pp = lanes(loop(local_cols, direct, zero, unroll=2))
            rr = norm
    gap_ref[...] = jnp.sqrt(gap_total(2) / mean_of)


def on_device(
    tile_data, tile_row, tile_col, tile_count, touched, owner_map, observed, start_x, start_u
):
    nd, n = lax.axis_size(AXES[0]), lax.axis_size(AXES[1])
    shards = nd * n
    local_cols = touched.shape[1]
    col_blocks = owner_map.shape[0]
    cb = col_blocks // shards
    row_blocks = observed.shape[0]
    slots, blk, _ = tile_data.shape
    targets = start_x.shape[2]
    subs = targets // PIECE
    f32, b16, i32 = jnp.float32, jnp.bfloat16, jnp.int32
    shape = jax.ShapeDtypeStruct
    assert nd == 2 * n * n and shards == 128 and col_blocks == cb * shards
    assert max(local_cols, slots, row_blocks) <= blk and targets % PIECE == 0

    md, mk = lax.axis_index(AXES[0]), lax.axis_index(AXES[1])
    wanted = touched[0]
    matches = wanted[:, None] == jnp.arange(col_blocks, dtype=i32)[None, :]
    position = jnp.sum(jnp.where(matches, owner_map[None, :], 0), axis=1)
    owner = position // cb
    local_slot = position - owner * cb
    away = {
        "z": (owner % n - mk) % n,
        "x": ((owner // (2 * n)) % n - (md // 2) % n) % n,
        "y": (owner // (2 * n * n) - md // (2 * n)) % n,
    }
    core = (owner // n + md) % 2
    mail = jnp.stack(
        [((core * n + away[a]) * n + away[b]) * n + away[c] for a, b, c in ORDERS]
    )
    hit = mail[:, :, None] == jnp.arange(shards, dtype=i32)[None, None, :]
    column = jnp.arange(local_cols, dtype=i32)
    slot_of = jnp.sum(jnp.where(hit, column[None, :, None], 0), axis=1)
    tags = jnp.sum(jnp.where(hit, local_slot[None, :, None] + 1, 0), axis=1) - 1
    tags = jnp.broadcast_to(tags.astype(f32)[:, :, None], (3, shards, blk))

    number = jnp.arange(slots, dtype=i32)
    used = number < tile_count[0]

    def sorting(keys, values, bins):
        keys = jnp.where(used, keys, bins)
        full = keys * slots + number
        before = full[None, :] < full[:, None]
        rank = jnp.sum(before.astype(i32), axis=1)
        same = before & (keys[None, :] == keys[:, None])
        first = 1 - jnp.max(same.astype(i32), axis=1)
        landed = rank[None, :] == number[:, None]
        pick = lambda v: jnp.sum(jnp.where(landed, v[None, :], 0), axis=1)
        bin_of = jnp.arange(bins, dtype=i32)
        upto = jnp.sum((keys[None, :] <= bin_of[:, None]).astype(i32), axis=1)
        some = jnp.max((keys[None, :] == bin_of[:, None]).astype(i32), axis=1)
        return pick(number), pick(values), pick(first), jnp.where(some > 0, upto - 1, slots)

    row, col = tile_row[0], tile_col[0]
    ftile, ffrom, ffirst, row_last = sorting(row, col, row_blocks)
    btile, bfrom, bfirst, col_last = sorting(col, row, local_cols)

    def padded(v):
        return jnp.pad(v, (0, blk - v.shape[0]))[None, :]

    table = jnp.concatenate(
        [slot_of, jnp.pad(mail, ((0, 0), (0, blk - local_cols)))]
        + [padded(v) for v in (ftile, ffrom, ffirst, btile, bfrom, bfirst, row_last, col_last)],
        axis=0,
    )

    x = jnp.swapaxes(start_x, 1, 2)
    u = jnp.swapaxes(start_u, 1, 2)
    obs = jnp.swapaxes(observed, 1, 2)
    vec = (local_cols, targets, blk)
    pieces = lambda *lead: pltpu.VMEM((*lead, PIECE, blk), f32)
    dma = lambda *count: pltpu.SemaphoreType.DMA(count)
    plane, groups, ring = n * n, 2 * n, n * cb
    vm = pl.BlockSpec(memory_space=pltpu.VMEM)
    hbm = pl.BlockSpec(memory_space=pltpu.HBM)
    x, u, zown, gap = pl.pallas_call(
        functools.partial(kernel, n, cb, shards * local_cols * blk),
        out_shape=(
            shape(vec, f32), shape(vec, f32), shape((cb, targets, blk), f32),
            shape((PIECE, blk), f32),
        ),
        in_specs=[pl.BlockSpec(memory_space=pltpu.SMEM), vm, hbm, hbm, hbm, hbm],
        out_specs=(vm,) * 4,
        scratch_shapes=[
            pltpu.VMEM((slots, blk, blk), f32),
            pltpu.VMEM((row_blocks, targets, blk), f32),
            pltpu.VMEM((slots, 2 * blk, blk), b16),
            pltpu.VMEM((slots, 2 * blk, blk), b16),
            pltpu.VMEM((local_cols, 2 * targets, blk), b16),
            pltpu.VMEM((row_blocks, 2 * targets, blk), b16),
            pltpu.VMEM((slots + 1, targets, blk), f32),
            pltpu.VMEM((slots + 1, targets, blk), f32),
            pltpu.VMEM(vec, f32), pltpu.VMEM(vec, f32), pltpu.VMEM(vec, f32),
            pieces(subs, shards), pieces(subs, shards),
            pieces(subs + 1, plane * cb), pieces(subs + 1, plane * cb),
            pieces(subs + 1, ring), pieces(subs + 1, ring),
            pieces(subs, ring), pieces(subs, plane * cb),
            pieces(subs, shards), pieces(subs, shards),
            pltpu.VMEM((3, shards, blk), f32), pieces(3, shards),
            pieces(cb), pieces(3, groups),
            dma(4), dma(subs), dma(subs),
            dma(subs + 1), dma(subs + 1), dma(subs + 1), dma(subs + 1),
            dma(subs), dma(subs), dma(subs), dma(subs), dma(subs), dma(subs),
            dma(3), dma(3), dma(3), dma(3),
        ],
        compiler_params=pltpu.CompilerParams(
            vmem_limit_bytes=VMEM_MIB * MIB, has_side_effects=True, collective_id=0
        ),
        name="admm",
    )(table, tags, tile_data, obs, x, u)
    primal_gap = gap[0, :targets]
    return (jnp.swapaxes(x, 1, 2), jnp.swapaxes(u, 1, 2), jnp.swapaxes(zown, 1, 2), primal_gap)


def solution(mesh):
    both = P(AXES)
    placed = (
        P(AXES, None, None), P(AXES, None), P(AXES, None), both, P(AXES, None), P(),
        P(AXES, None, None), P(AXES, None, None), P(AXES, None, None),
    )
    return jax.shard_map(
        on_device,
        mesh=mesh,
        in_specs=placed,
        out_specs=(P(AXES, None, None), P(AXES, None, None), P(AXES, None, None), P()),
        check_vma=False,
    )
```

```python
import functools

import jax
import jax.numpy as jnp
from jax import lax
from jax.experimental import pallas as pl
from jax.experimental.pallas import tpu as pltpu
from jax.sharding import PartitionSpec as P

ITERS = 2
CG_STEPS = 4
PENALTY = 1.0
COUPLING = 1.0
AXES = ("dev", "ka")
MESH = pl.DeviceIdType.MESH
MIB = 1 << 20
VMEM_MIB = 48
PIECE = 8
ORDERS = ("xzy", "yxz", "zyx", "yzx")
SUB_ORDER = (0, 1, 2, 0, 1, 2, 0, 3)
KINDS = len(ORDERS)
SLOT, MAIL, FWD_TILE, FWD_FROM, FWD_FIRST, BWD_TILE, BWD_FROM, BWD_FIRST, ROW_LAST, COL_LAST = (
    0, 4, 8, 9, 10, 11, 12, 13, 14, 15,
)
FIRST_PLAN = (
    7, 3, 6, 5, 1, 90, 2, 4, 0, 13, 91, 17, 15, 11, 92, 16, 12, 93, 14, 10, 25, 27, 21, 26,
    23, 22, 24, 20, 35, 31, 36, 37, 33, 32, 34, 30, 45, 41, 46, 44, 42, 43, 40, 47, 51, 56,
    52, 54, 50, 57, 55, 53,
)
NEXT_PLAN = (
    0, 4, 5, 90, 7, 2, 3, 10, 1, 6, 15, 17, 14, 13, 12, 16, 11, 24, 20, 23, 25, 27, 22, 21,
    26, 30, 34, 35, 33, 37, 32, 31, 36, 44, 40, 45, 41, 43, 42, 47, 46, 54, 50, 51, 55, 53,
    52, 57, 56,
)


def split(value):
    high = value.astype(jnp.bfloat16)
    low = (value - high.astype(jnp.float32)).astype(jnp.bfloat16)
    return jnp.concatenate([high, low], axis=0)


def lanes(total):
    return jnp.sum(total, axis=1, keepdims=True)


def kernel(
    n, cb, mean_of,
    tab, tags_ref, tile_hbm, obs_hbm, x_hbm, u_hbm,
    x_ref, u_ref, zown_ref, gap_ref,
    tile_ref, obs_ref, fwd_ref, bwd_ref, pb_ref, wb_ref, wseg, qseg, r_ref, p_ref, zu_ref,
    box, in1, sum1, in2, sum2, in3, zz2, zz1, zbox, tagin, tagx, share_ref, gin, cin,
    load_sem, r1_s, r1_r, r2_s, r2_r, r3_s, r3_r, b3_s, b3_r, b2_s, b2_r, b1_s, b1_r,
    tag_s, tag_r, gap_s, gap_r, cnt_s, cnt_r,
):
    slots, blk, _ = tile_ref.shape
    local_cols, targets, _ = x_ref.shape
    row_blocks = obs_ref.shape[0]
    subs = targets // PIECE
    plane = n * n
    groups = 2 * n
    f32 = jnp.float32
    md, mk = lax.axis_index(AXES[0]), lax.axis_index(AXES[1])
    at = {"c": lax.rem(md, 2), "x": lax.rem(md // 2, n), "y": md // (2 * n), "z": mk}

    def device(axis, da, dc=0):
        place = dict(at)
        place[axis] = lax.rem(place[axis] + da, n)
        place["c"] = lax.rem(place["c"] + dc, 2)
        return ((place["y"] * n + place["x"]) * 2 + place["c"], place["z"])

    def remote(source, target, send_sem, recv_sem, where):
        return pltpu.make_async_remote_copy(
            source, target, send_sem, recv_sem, device_id=where, device_id_type=MESH
        )

    def order(k):
        return SUB_ORDER[k]

    def axis(k, level):
        return ORDERS[order(k)][level]

    def back(da):
        return (n - da) % n

    line = [(dc, da) for dc in range(2) for da in range(n)][1:]
    anyone = device("x", 1)

    def line_sends(k, p, source, target, send_sem, recv_sem):
        for dc, da in line:
            mine, theirs = (dc * n + da) * plane, (dc * n + back(da)) * plane
            remote(
                source.at[k, pl.ds(mine, plane)], target.at[k, pl.ds(theirs, plane)],
                send_sem.at[k], recv_sem.at[k], device(ORDERS[p][0], da, dc),
            ).start()

    def ring_sends(k, where, pick, size, source, target, send_sem, recv_sem):
        for da in range(1, n):
            remote(
                source.at[k, pl.ds(da * size if pick else 0, size)],
                target.at[k, pl.ds(back(da) * size, size)],
                send_sem.at[k], recv_sem.at[k], device(where, da),
            ).start()

    def rest(ref, k, size):
        return ref.at[k, pl.ds(size, ref.shape[1] - size)]

    def arrived(ref, k, size, sems):
        part = rest(ref, k, size)
        remote(part, part, sems[0].at[k], sems[1].at[k], anyone).wait_recv()

    def left(ref, k, size, sems):
        part = rest(ref, k, size)
        remote(part, part, sems[0].at[k], sems[1].at[k], anyone).wait_send()

    r1, r2, r3 = (r1_s, r1_r), (r2_s, r2_r), (r3_s, r3_r)
    b3, b2, b1 = (b3_s, b3_r), (b2_s, b2_r), (b1_s, b1_r)
    tagged = (tag_s, tag_r)

    greeted = [device(ORDERS[0][0], da, dc) for dc, da in line]
    for where in ORDERS[0][1:]:
        greeted += [device(where, da, dc) for dc in range(2) for da in range(1, n)]
    barrier = pltpu.get_barrier_semaphore()
    for where in greeted:
        pl.semaphore_signal(barrier, inc=1, device_id=where, device_id_type=MESH)

    loads = [
        pltpu.make_async_copy(source, target, load_sem.at[i])
        for i, (source, target) in enumerate(
            ((x_hbm, x_ref), (u_hbm, u_ref), (tile_hbm, tile_ref), (obs_hbm, obs_ref))
        )
    ]
    for one in loads:
        one.start()

    def members(p):
        return [k for k in range(subs) if order(k) == p]

    def build(p):
        def one(i, carry):
            for g in range(groups):
                q = g * plane + i
                slot = tab[SLOT + p, q]
                for k in members(p):
                    rows = pl.ds(k * PIECE, PIECE)
                    box[k, q] = x_ref[slot, rows] + u_ref[slot, rows]
            return carry

        lax.fori_loop(0, plane, one, 0)

    def send_r1(k):
        line_sends(k, order(k), box, in1, *r1)

    def send_r2(k):
        ring_sends(k, axis(k, 1), True, n * cb, sum1, in2, *r2)

    def t1(k):
        p = order(k)
        arrived(in1, k, plane, r1)

        def one(i, carry):
            total = [jnp.zeros((PIECE, blk), f32)] * cb
            for s in range(groups):
                value = box[k, i] if s == 0 else in1[k, s * plane + i]
                tag = tagx[p, i * groups + s]
                total = [t + jnp.where(tag == b, value, 0.0) for b, t in enumerate(total)]
            for b in range(cb):
                sum1[k, i * cb + b] = total[b]
            return carry

        lax.fori_loop(0, plane, one, 0, unroll=2)
        send_r2(k)

    def t2(k):
        size = n * cb
        arrived(in2, k, size, r2)
        for j in range(size):
            total = sum1[k, j]
            for s in range(1, n):
                total = total + in2[k, s * size + j]
            sum2[k, j] = total
        ring_sends(k, axis(k, 2), True, cb, sum2, in3, *r3)

    def total3(k, b):
        total = sum2[k, b]
        for s in range(1, n):
            total = total + in3[k, s * cb + b]
        return total

    def t3(k):
        arrived(in3, k, cb, r3)
        for b in range(cb):
            share = share_ref[b]
            amount = total3(k, b) / share
            cutoff = PENALTY / (COUPLING * share)
            z = amount - jnp.clip(amount, -cutoff, cutoff)
            zz2[k, b] = z
            zown_ref[b, pl.ds(k * PIECE, PIECE)] = z
        ring_sends(k, axis(k, 2), False, cb, zz2, zz2, *b3)

    def t4(k):
        arrived(zz2, k, cb, b3)
        for j in range(n * cb):
            zz1[k, j] = zz2[k, j]
        ring_sends(k, axis(k, 1), False, n * cb, zz2, zz1, *b2)

    def t5(k):
        p = order(k)
        arrived(zz1, k, n * cb, b2)
        left(box, k, plane, r1)

        def one(i, carry):
            z = [zz1[k, i * cb + b] for b in range(cb)]
            for s in range(groups):
                tag = tagx[p, i * groups + s]
                value = z[cb - 1]
                for b in range(cb - 1):
                    value = jnp.where(tag == b, z[b], value)
                if s == 0:
                    zbox[k, i] = value
                else:
                    box[k, s * plane + i] = value
            return carry

        lax.fori_loop(0, plane, one, 0, unroll=2)
        line_sends(k, p, box, zbox, *b1)

    def start_exchange():
        for p in range(KINDS):
            build(p)

    def exchange(plan, works):
        tasks = (send_r1, t1, t2, t3, t4, t5)
        for step in plan:
            level, k = divmod(step, 10)
            if level == 9:
                works[k]()
            else:
                tasks[level](k)
        for k in range(subs):
            arrived(zbox, k, plane, b1)
        for k in range(subs):
            left(sum1, k, n * cb, r2)
            left(sum2, k, cb, r3)
            left(in3, k, cb, b3)
            left(zz1, k, n * cb, b2)
            left(box, k, plane, b1)

    def tile_pass(tiles_ref, from_row, first_row, source_ref, seg_ref):
        group = min(16, slots)

        def step(number, total):
            for inner in range(group):
                t = number * group + inner
                lhs = source_ref[tab[from_row, t]]
                out = jnp.dot(
                    jnp.concatenate([lhs, lhs], axis=1), tiles_ref[t],
                    preferred_element_type=f32,
                )
                fresh = tab[first_row, t] == 1
                total = jnp.where(fresh, 0.0, total) + (out[:targets] + out[targets:])
                seg_ref[t] = total
            return total

        lax.fori_loop(0, slots // group, step, jnp.zeros((targets, blk), f32))

    def forward():
        tile_pass(fwd_ref, FWD_FROM, FWD_FIRST, pb_ref, wseg)

    def backward():
        tile_pass(bwd_ref, BWD_FROM, BWD_FIRST, wb_ref, qseg)

    def loop(count, body, init=0, unroll=4):
        return lax.fori_loop(0, count, body, init, unroll=unroll)

    zero = jnp.zeros((targets, blk), f32)
    wseg[slots] = zero
    qseg[slots] = zero

    loads[0].wait()
    loads[1].wait()
    start_exchange()
    pl.semaphore_wait(barrier, len(greeted))
    for p in range(KINDS):
        for dc, da in line:
            remote(
                tags_ref.at[p, pl.ds(dc * n + da, 1)],
                tagin.at[p, pl.ds(dc * n + back(da), 1)],
                tag_s.at[p], tag_r.at[p], device(ORDERS[p][0], da, dc),
            ).start()

    lane = lax.broadcasted_iota(jnp.int32, (PIECE, blk), 1)

    def count_send(stage):
        ring_sends(stage, ORDERS[0][stage + 1], False, 1, cin, cin, cnt_s, cnt_r)

    def count_total(stage, size):
        arrived(cin, stage, 1, (cnt_s, cnt_r))
        left(cin, stage, 1, (cnt_s, cnt_r))
        total = cin[stage, 0]
        for s in range(1, n):
            total = total + pltpu.roll(cin[stage, s], blk - back(s) * size, 1)
        return total

    def learn():
        for p in range(KINDS):
            tagin[p, 0] = tags_ref[p, 0]
            arrived(tagin, p, 1, tagged)
            left(tagin, p, 1, tagged)

            def expand(s, carry):
                row = tagin[p, s]
                for i in range(plane):
                    tagx[p, i * groups + s] = jnp.broadcast_to(row[:, i : i + 1], (PIECE, blk))
                return carry

            loop(groups, expand, unroll=1)

        def census(i, held):
            total = [jnp.zeros((PIECE, blk), f32)] * cb
            for s in range(groups):
                tag = tagx[0, i * groups + s]
                total = [t + jnp.where(tag == b, 1.0, 0.0) for b, t in enumerate(total)]
            for b in range(cb):
                held = jnp.where(lane == i * cb + b, total[b], held)
            return held

        cin[0, 0] = loop(plane, census, jnp.zeros((PIECE, blk), f32), unroll=1)
        count_send(0)

    def ready():
        def opening(c, carry):
            pb_ref[c] = split(x_ref[c])
            return carry

        loop(local_cols, opening)
        loads[2].wait()

        def convert(t, carry):
            fwd_ref[t] = split(tile_ref[tab[FWD_TILE, t]].T)
            bwd_ref[t] = split(tile_ref[tab[BWD_TILE, t]])
            return carry

        loop(slots, convert)
        cin[1, 0] = count_total(0, n * cb)
        count_send(1)

    def towards():
        forward()
        loads[3].wait()

        def against(r, carry):
            wb_ref[r] = split(obs_ref[r] - wseg[tab[ROW_LAST, r]])
            return carry

        loop(row_blocks, against)
        total = count_total(1, cb)
        for b in range(cb):
            share = jnp.maximum(total[:, b : b + 1], 1.0)
            share_ref[b] = jnp.broadcast_to(share, (PIECE, blk))

    def basis():
        backward()

        def one(c, carry):
            r_ref[c] = qseg[tab[COL_LAST, c]] - COUPLING * x_ref[c]
            return carry

        loop(local_cols, one)

    exchange(FIRST_PLAN, (learn, ready, towards, basis))

    gap_line = ORDERS[0]

    def gap_send(stage):
        if stage == 0:
            for dc, da in line:
                remote(
                    gin.at[0, pl.ds(0, 1)], gin.at[0, pl.ds(dc * n + back(da), 1)],
                    gap_s.at[0], gap_r.at[0], device(gap_line[0], da, dc),
                ).start()
        else:
            ring_sends(stage, gap_line[stage], False, 1, gin, gin, gap_s, gap_r)

    def gap_total(stage):
        count = groups if stage == 0 else n
        part = gin.at[stage, pl.ds(1, count - 1)]
        one = remote(part, part, gap_s.at[stage], gap_r.at[stage], anyone)
        one.wait_recv()
        one.wait_send()
        total = gin[stage, 0]
        for s in range(1, count):
            total = total + gin[stage, s]
        return total

    for outer_step in range(ITERS):
        last = outer_step == ITERS - 1

        def begin(c, carry):
            rr, gap = carry
            z = jnp.concatenate(
                [zbox[k, tab[MAIL + order(k), c]] for k in range(subs)], axis=0
            )
            d = x_ref[c] - z
            u = u_ref[c] + d
            u_ref[c] = u
            zu = z - u
            r = r_ref[c] + COUPLING * zu
            r_ref[c] = r
            p_ref[c] = r
            pb_ref[c] = split(r)
            if last:
                gap = gap + d * d
            else:
                zu_ref[c] = zu
            return rr + r * r, gap

        rr, gap = loop(local_cols, begin, (zero, zero), unroll=2)
        rr = lanes(rr)
        pp = rr
        if last:
            gin[0, 0] = lax.dot_general(
                jnp.ones((PIECE, blk), f32),
                jnp.concatenate([gap, jnp.zeros((blk - targets, blk), f32)], axis=0),
                (((1,), (1,)), ((), ())),
                precision=lax.Precision.HIGHEST, preferred_element_type=f32,
            )
            gap_send(0)

        for step in range(CG_STEPS):
            closing = step == CG_STEPS - 1
            forward()

            def image(i, ww):
                w = wseg[tab[ROW_LAST, i]]
                if not (last and closing):
                    wb_ref[i] = split(w)
                return ww + w * w

            ww = lanes(loop(row_blocks, image, zero))
            size = rr / (ww + COUPLING * pp)
            if closing:

                def finish(c, carry):
                    x_ref[c] = x_ref[c] + size * p_ref[c]
                    return carry

                loop(local_cols, finish)
                if last:
                    break
                start_exchange()

                def rest_of_step():
                    backward()

                    def close(c, carry):
                        q = qseg[tab[COL_LAST, c]] + COUPLING * p_ref[c]
                        r_ref[c] = r_ref[c] - size * q - COUPLING * zu_ref[c]
                        return carry

                    loop(local_cols, close)

                exchange(NEXT_PLAN, (rest_of_step,))
                break
            backward()
            if last and step < 2:
                gin[step + 1, 0] = gap_total(step)
                gap_send(step + 1)

            def reduce(c, total):
                q = qseg[tab[COL_LAST, c]] + COUPLING * p_ref[c]
                r = r_ref[c] - size * q
                r_ref[c] = r
                return total + r * r

            norm = lanes(loop(local_cols, reduce, zero))
            turn = norm / rr

            def direct(c, total):
                old = p_ref[c]
                x_ref[c] = x_ref[c] + size * old
                p = r_ref[c] + turn * old
                p_ref[c] = p
                pb_ref[c] = split(p)
                return total + p * p

            pp = lanes(loop(local_cols, direct, zero, unroll=2))
            rr = norm
    gap_ref[...] = jnp.sqrt(gap_total(2) / mean_of)


def deliver_kernel(x_ref, u_ref, z_ref, gap_ref, x_hbm, u_hbm, z_hbm, out_ref, sems):
    copies = [
        pltpu.make_async_copy(source, target, sems.at[i])
        for i, (source, target) in enumerate(((x_ref, x_hbm), (u_ref, u_hbm), (z_ref, z_hbm)))
    ]
    for one in copies:
        one.start()
    out_ref[...] = gap_ref[0, : out_ref.shape[0]]
    for one in copies:
        one.wait()


def on_device(
    tile_data, tile_row, tile_col, tile_count, touched, owner_map, observed, start_x, start_u
):
    nd, n = lax.axis_size(AXES[0]), lax.axis_size(AXES[1])
    shards = nd * n
    local_cols = touched.shape[1]
    col_blocks = owner_map.shape[0]
    cb = col_blocks // shards
    row_blocks = observed.shape[0]
    slots, blk, _ = tile_data.shape
    targets = start_x.shape[2]
    subs = targets // PIECE
    plane, groups, ring = n * n, 2 * n, n * cb
    f32, b16, i32 = jnp.float32, jnp.bfloat16, jnp.int32
    shape = jax.ShapeDtypeStruct
    assert nd == 2 * n * n and shards == 128 and subs == len(SUB_ORDER)
    assert max(local_cols, slots, row_blocks) <= blk and targets % PIECE == 0

    md, mk = lax.axis_index(AXES[0]), lax.axis_index(AXES[1])
    wanted = touched[0]
    matches = wanted[:, None] == jnp.arange(col_blocks, dtype=i32)[None, :]
    position = jnp.sum(jnp.where(matches, owner_map[None, :], 0), axis=1)
    owner = position // cb
    local_slot = position - owner * cb
    away = {
        "z": (owner % n - mk) % n,
        "x": ((owner // (2 * n)) % n - (md // 2) % n) % n,
        "y": (owner // (2 * n * n) - md // (2 * n)) % n,
    }
    core = (owner // n + md) % 2
    mail = jnp.stack(
        [((core * n + away[a]) * n + away[b]) * n + away[c] for a, b, c in ORDERS]
    )
    hit = mail[:, :, None] == jnp.arange(shards, dtype=i32)[None, None, :]
    column = jnp.arange(local_cols, dtype=i32)
    slot_of = jnp.sum(jnp.where(hit, column[None, :, None], 0), axis=1)
    tags = jnp.sum(jnp.where(hit, local_slot[None, :, None] + 1, 0), axis=1) - 1
    tags = tags.astype(f32).reshape(KINDS, groups, 1, plane)
    tags = jnp.pad(tags, ((0, 0), (0, 0), (0, 0), (0, blk - plane)))
    tags = jnp.broadcast_to(tags, (KINDS, groups, PIECE, blk))

    number = jnp.arange(slots, dtype=i32)
    used = number < tile_count[0]

    def sorting(keys, values, bins):
        keys = jnp.where(used, keys, bins)
        full = keys * slots + number
        before = full[None, :] < full[:, None]
        rank = jnp.sum(before.astype(i32), axis=1)
        same = before & (keys[None, :] == keys[:, None])
        first = 1 - jnp.max(same.astype(i32), axis=1)
        landed = rank[None, :] == number[:, None]
        pick = lambda v: jnp.sum(jnp.where(landed, v[None, :], 0), axis=1)
        bin_of = jnp.arange(bins, dtype=i32)
        upto = jnp.sum((keys[None, :] <= bin_of[:, None]).astype(i32), axis=1)
        some = jnp.max((keys[None, :] == bin_of[:, None]).astype(i32), axis=1)
        return pick(number), pick(values), pick(first), jnp.where(some > 0, upto - 1, slots)

    row, col = tile_row[0], tile_col[0]
    ftile, ffrom, ffirst, row_last = sorting(row, col, row_blocks)
    btile, bfrom, bfirst, col_last = sorting(col, row, local_cols)

    def padded(v):
        return jnp.pad(v, (0, blk - v.shape[0]))[None, :]

    table = jnp.concatenate(
        [slot_of, jnp.pad(mail, ((0, 0), (0, blk - local_cols)))]
        + [padded(v) for v in (ftile, ffrom, ffirst, btile, bfrom, bfirst, row_last, col_last)],
        axis=0,
    )

    x = jnp.swapaxes(start_x, 1, 2)
    u = jnp.swapaxes(start_u, 1, 2)
    obs = jnp.swapaxes(observed, 1, 2)
    vec = (local_cols, targets, blk)
    pieces = lambda *lead: pltpu.VMEM((*lead, PIECE, blk), f32)
    dma = lambda *count: pltpu.SemaphoreType.DMA(count)
    vm = pl.BlockSpec(memory_space=pltpu.VMEM)
    hbm = pl.BlockSpec(memory_space=pltpu.HBM)
    x, u, zown, gap = pl.pallas_call(
        functools.partial(kernel, n, cb, shards * local_cols * blk),
        out_shape=(
            shape(vec, f32), shape(vec, f32), shape((cb, targets, blk), f32),
            shape((PIECE, blk), f32),
        ),
        in_specs=[pl.BlockSpec(memory_space=pltpu.SMEM), vm, hbm, hbm, hbm, hbm],
        out_specs=(vm,) * 4,
        scratch_shapes=[
            pltpu.VMEM((slots, blk, blk), f32),
            pltpu.VMEM((row_blocks, targets, blk), f32),
            pltpu.VMEM((slots, 2 * blk, blk), b16),
            pltpu.VMEM((slots, 2 * blk, blk), b16),
            pltpu.VMEM((local_cols, 2 * targets, blk), b16),
            pltpu.VMEM((row_blocks, 2 * targets, blk), b16),
            pltpu.VMEM((slots + 1, targets, blk), f32),
            pltpu.VMEM((slots + 1, targets, blk), f32),
            pltpu.VMEM(vec, f32), pltpu.VMEM(vec, f32), pltpu.VMEM(vec, f32),
            pieces(subs, shards), pieces(subs, shards),
            pieces(subs, plane * cb), pieces(subs, plane * cb),
            pieces(subs, ring), pieces(subs, ring),
            pieces(subs, ring), pieces(subs, plane * cb),
            pieces(subs, shards),
            pieces(KINDS, groups), pieces(KINDS, shards),
            pieces(cb), pieces(3, groups), pieces(2, n),
            dma(4), dma(subs), dma(subs),
            dma(subs), dma(subs), dma(subs), dma(subs),
            dma(subs), dma(subs), dma(subs), dma(subs), dma(subs), dma(subs),
            dma(KINDS), dma(KINDS), dma(3), dma(3), dma(2), dma(2),
        ],
        compiler_params=pltpu.CompilerParams(
            vmem_limit_bytes=VMEM_MIB * MIB, has_side_effects=True, collective_id=0
        ),
        name="admm",
    )(table, tags, tile_data, obs, x, u)
    x, u, zown, primal_gap = pl.pallas_call(
        deliver_kernel,
        out_shape=(
            shape(vec, f32), shape(vec, f32), shape((cb, targets, blk), f32),
            shape((targets,), f32),
        ),
        in_specs=[vm] * 4,
        out_specs=(hbm, hbm, hbm, vm),
        scratch_shapes=[dma(3)],
        compiler_params=pltpu.CompilerParams(vmem_limit_bytes=MIB),
        name="deliver",
    )(x, u, zown, gap)
    return (jnp.swapaxes(x, 1, 2), jnp.swapaxes(u, 1, 2), jnp.swapaxes(zown, 1, 2), primal_gap)


def solution(mesh):
    both = P(AXES)
    placed = (
        P(AXES, None, None), P(AXES, None), P(AXES, None), both, P(AXES, None), P(),
        P(AXES, None, None), P(AXES, None, None), P(AXES, None, None),
    )
    return jax.shard_map(
        on_device,
        mesh=mesh,
        in_specs=placed,
        out_specs=(P(AXES, None, None), P(AXES, None, None), P(AXES, None, None), P()),
        check_vma=False,
    )
```

```python
import functools

import jax
import jax.numpy as jnp
from jax import lax
from jax.experimental import pallas as pl
from jax.experimental.pallas import tpu as pltpu
from jax.sharding import PartitionSpec as P

ITERS = 2
CG_STEPS = 4
PENALTY = 1.0
COUPLING = 1.0
AXES = ("dev", "ka")
MESH = pl.DeviceIdType.MESH
MIB = 1 << 20
VMEM_MIB = 48
PIECE = 8
ORDERS = ("xzy", "yxz", "zyx", "yzx")
SUB_ORDER = (0, 1, 2, 0, 1, 2, 0, 3)
KINDS = len(ORDERS)
SLOT, MAIL, FWD_TILE, FWD_FROM, FWD_FIRST, BWD_TILE, BWD_FROM, BWD_FIRST, ROW_LAST, COL_LAST = (
    0, 4, 8, 9, 10, 11, 12, 13, 14, 15,
)
FIRST_PLAN = (
    7, 3, 6, 5, 1, 90, 2, 4, 0, 13, 91, 17, 15, 11, 92, 16, 12, 93, 14, 10, 25, 27, 21, 26,
    23, 22, 24, 20, 35, 31, 36, 37, 33, 32, 34, 30, 45, 41, 46, 44, 42, 43, 40, 47, 51, 56,
    52, 54, 50, 57, 55, 53,
)
NEXT_PLAN = (
    0, 4, 5, 90, 7, 2, 3, 10, 1, 6, 15, 17, 14, 13, 12, 16, 11, 24, 20, 23, 25, 27, 22, 21,
    26, 30, 34, 35, 33, 37, 32, 31, 36, 44, 40, 45, 41, 43, 42, 47, 46, 54, 50, 51, 55, 53,
    52, 57, 56,
)


def split(value):
    high = value.astype(jnp.bfloat16)
    low = (value - high.astype(jnp.float32)).astype(jnp.bfloat16)
    return jnp.concatenate([high, low], axis=0)


def lanes(total):
    return jnp.sum(total, axis=1, keepdims=True)


def kernel(
    n, cb, mean_of,
    raw_ref, tile_hbm, obs_hbm, x_hbm, u_hbm,
    x_ref, u_ref, zown_ref, gap_ref,
    lists, tab, tags_ref, tile_ref, fwd_ref, bwd_ref, pb_ref, wb_ref, wseg, qseg, r_ref, p_ref, zu_ref,
    box, in1, sum1, in2, sum2, in3, zz2, zz1, zbox, tagin, tagx, share_ref, gin, cin,
    load_sem, tab_sem, r1_s, r1_r, r2_s, r2_r, r3_s, r3_r, b3_s, b3_r, b2_s, b2_r, b1_s, b1_r,
    tag_s, tag_r, gap_s, gap_r, cnt_s, cnt_r,
):
    slots, blk, _ = tile_ref.shape
    local_cols, targets, _ = x_ref.shape
    row_blocks = obs_hbm.shape[0]
    obs_ref = zu_ref.at[pl.ds(0, row_blocks)]
    subs = targets // PIECE
    plane = n * n
    groups = 2 * n
    f32 = jnp.float32
    md, mk = lax.axis_index(AXES[0]), lax.axis_index(AXES[1])
    at = {"c": lax.rem(md, 2), "x": lax.rem(md // 2, n), "y": md // (2 * n), "z": mk}

    def device(axis, da, dc=0):
        place = dict(at)
        place[axis] = lax.rem(place[axis] + da, n)
        place["c"] = lax.rem(place["c"] + dc, 2)
        return ((place["y"] * n + place["x"]) * 2 + place["c"], place["z"])

    def remote(source, target, send_sem, recv_sem, where):
        return pltpu.make_async_remote_copy(
            source, target, send_sem, recv_sem, device_id=where, device_id_type=MESH
        )

    def order(k):
        return SUB_ORDER[k]

    def axis(k, level):
        return ORDERS[order(k)][level]

    def back(da):
        return (n - da) % n

    line = [(dc, da) for dc in range(2) for da in range(n)][1:]
    anyone = device("x", 1)

    def line_sends(k, p, source, target, send_sem, recv_sem):
        for dc, da in line:
            mine, theirs = (dc * n + da) * plane, (dc * n + back(da)) * plane
            remote(
                source.at[k, pl.ds(mine, plane)], target.at[k, pl.ds(theirs, plane)],
                send_sem.at[k], recv_sem.at[k], device(ORDERS[p][0], da, dc),
            ).start()

    def ring_sends(k, where, pick, size, source, target, send_sem, recv_sem):
        for da in range(1, n):
            remote(
                source.at[k, pl.ds(da * size if pick else 0, size)],
                target.at[k, pl.ds(back(da) * size, size)],
                send_sem.at[k], recv_sem.at[k], device(where, da),
            ).start()

    def rest(ref, k, size):
        return ref.at[k, pl.ds(size, ref.shape[1] - size)]

    def arrived(ref, k, size, sems):
        part = rest(ref, k, size)
        remote(part, part, sems[0].at[k], sems[1].at[k], anyone).wait_recv()

    def left(ref, k, size, sems):
        part = rest(ref, k, size)
        remote(part, part, sems[0].at[k], sems[1].at[k], anyone).wait_send()

    r1, r2, r3 = (r1_s, r1_r), (r2_s, r2_r), (r3_s, r3_r)
    b3, b2, b1 = (b3_s, b3_r), (b2_s, b2_r), (b1_s, b1_r)
    tagged = (tag_s, tag_r)

    greeted = [device(ORDERS[0][0], da, dc) for dc, da in line]
    for where in ORDERS[0][1:]:
        greeted += [device(where, da, dc) for dc in range(2) for da in range(1, n)]
    barrier = pltpu.get_barrier_semaphore()
    for where in greeted:
        pl.semaphore_signal(barrier, inc=1, device_id=where, device_id_type=MESH)

    loads = [
        pltpu.make_async_copy(source, target, load_sem.at[i])
        for i, (source, target) in enumerate(
            ((x_hbm, x_ref), (u_hbm, u_ref), (tile_hbm, tile_ref), (obs_hbm, obs_ref))
        )
    ]
    loads[0].start()
    loads[1].start()

    def line_of(row):
        return raw_ref[pl.ds(row, 1)].astype(f32)

    def spread(row):
        return jnp.broadcast_to(row, (blk, blk))

    def flip(row):
        return spread(row).T

    def tell(row, value):
        lists[pl.ds(row, 1)] = jnp.clip(value, 0.0, float(blk - 1)).astype(jnp.int32)

    def find(row, at_most, column):
        return jnp.clip(tab[row, column], 0, at_most)

    def publish(half):
        part = pl.ds(half * PIECE, PIECE)
        return pltpu.make_async_copy(lists.at[part], tab.at[part], tab_sem.at[half])

    down = lax.broadcasted_iota(jnp.int32, (blk, blk), 0).astype(f32)
    across = lax.broadcasted_iota(jnp.int32, (blk, blk), 1).astype(f32)
    none = jnp.zeros((blk, blk), f32)

    def place():
        wanted = flip(line_of(0))
        found = none
        for j in range(raw_ref.shape[0] - 4):
            hit = wanted == across + float(j * blk)
            found = found + jnp.where(hit, spread(line_of(4 + j)), 0.0)
        position = jnp.sum(found, axis=1, keepdims=True).astype(jnp.int32)
        owner = position // cb
        local_slot = (position % cb).astype(f32)
        away = {
            "z": (owner % n + n - at["z"]) % n,
            "x": ((owner // (2 * n)) % n + n - at["x"]) % n,
            "y": (owner // (2 * n * n) + n - at["y"]) % n,
        }
        core = (owner // n + at["c"]) % 2
        held = down < float(local_cols)
        for p, (first, second, third) in enumerate(ORDERS):
            mail = ((core * n + away[first]) * n + away[second]) * n + away[third]
            mail = jnp.broadcast_to(mail.astype(f32), (blk, blk))
            tell(MAIL + p, mail.T[:1])
            hit = held & (mail == across)
            tell(SLOT + p, jnp.max(jnp.where(hit, down, 0.0), axis=0, keepdims=True))
            tag = jnp.max(jnp.where(hit, local_slot + 1.0, 0.0), axis=0, keepdims=True) - 1.0
            tag = jnp.broadcast_to(tag, (PIECE, blk))
            for g in range(groups):
                turned = tag if g == 0 else pltpu.roll(tag, blk - g * plane, 1)
                tags_ref[p, g] = turned

    def sort_tiles(key_row, from_row, bins, first_table, last_table):
        count = line_of(3)
        number = across[:1]
        keys = jnp.where(number < count, line_of(key_row), float(bins))
        full = keys * float(blk) + number
        full_a, full_d = spread(full), flip(full)
        keys_a, keys_d = spread(keys), flip(keys)
        rank = jnp.sum(jnp.where(full_a < full_d, 1.0, 0.0), axis=1, keepdims=True)
        earlier = jnp.where((full_a < full_d) & (keys_a == keys_d), 1.0, 0.0)
        fresh = jnp.sum(earlier, axis=1, keepdims=True) == 0.0
        landed = rank == across

        def pick(value):
            return jnp.sum(jnp.where(landed, value, 0.0), axis=0, keepdims=True)

        tell(first_table, pick(down))
        tell(first_table + 1, pick(flip(line_of(from_row))))
        tell(first_table + 2, pick(jnp.where(fresh, 1.0, none)))
        upto = jnp.sum(jnp.where(keys_d <= across, 1.0, 0.0), axis=0, keepdims=True)
        some = jnp.sum(jnp.where(keys_d == across, 1.0, 0.0), axis=0, keepdims=True)
        tell(last_table, jnp.where(some > 0.0, upto - 1.0, float(slots)))

    place()
    publish(0).start()

    def members(p):
        return [k for k in range(subs) if order(k) == p]

    def build(p):
        def one(i, carry):
            for g in range(groups):
                q = g * plane + i
                slot = find(SLOT + p, local_cols - 1, q)
                for k in members(p):
                    rows = pl.ds(k * PIECE, PIECE)
                    box[k, q] = x_ref[slot, rows] + u_ref[slot, rows]
            return carry

        lax.fori_loop(0, plane, one, 0)

    built = set()

    def send_r1(k):
        if order(k) not in built:
            built.add(order(k))
            build(order(k))
        line_sends(k, order(k), box, in1, *r1)

    def send_r2(k):
        ring_sends(k, axis(k, 1), True, n * cb, sum1, in2, *r2)

    def t1(k):
        p = order(k)
        arrived(in1, k, plane, r1)

        def one(i, carry):
            total = [jnp.zeros((PIECE, blk), f32)] * cb
            for s in range(groups):
                value = box[k, i] if s == 0 else in1[k, s * plane + i]
                tag = tagx[p, i * groups + s]
                total = [t + jnp.where(tag == b, value, 0.0) for b, t in enumerate(total)]
            for b in range(cb):
                sum1[k, i * cb + b] = total[b]
            return carry

        lax.fori_loop(0, plane, one, 0, unroll=2)
        send_r2(k)

    def t2(k):
        size = n * cb
        arrived(in2, k, size, r2)
        for j in range(size):
            total = sum1[k, j]
            for s in range(1, n):
                total = total + in2[k, s * size + j]
            sum2[k, j] = total
        ring_sends(k, axis(k, 2), True, cb, sum2, in3, *r3)

    def total3(k, b):
        total = sum2[k, b]
        for s in range(1, n):
            total = total + in3[k, s * cb + b]
        return total

    def t3(k):
        arrived(in3, k, cb, r3)
        for b in range(cb):
            share = share_ref[b]
            amount = total3(k, b) / share
            cutoff = PENALTY / (COUPLING * share)
            z = amount - jnp.clip(amount, -cutoff, cutoff)
            zz2[k, b] = z
            zown_ref[b, pl.ds(k * PIECE, PIECE)] = z
        ring_sends(k, axis(k, 2), False, cb, zz2, zz2, *b3)

    def t4(k):
        arrived(zz2, k, cb, b3)
        for j in range(n * cb):
            zz1[k, j] = zz2[k, j]
        ring_sends(k, axis(k, 1), False, n * cb, zz2, zz1, *b2)

    def t5(k):
        p = order(k)
        arrived(zz1, k, n * cb, b2)
        left(box, k, plane, r1)

        def one(i, carry):
            z = [zz1[k, i * cb + b] for b in range(cb)]
            for s in range(groups):
                tag = tagx[p, i * groups + s]
                value = z[cb - 1]
                for b in range(cb - 1):
                    value = jnp.where(tag == b, z[b], value)
                if s == 0:
                    zbox[k, i] = value
                else:
                    box[k, s * plane + i] = value
            return carry

        lax.fori_loop(0, plane, one, 0, unroll=2)
        line_sends(k, p, box, zbox, *b1)

    def exchange(plan, works):
        tasks = (send_r1, t1, t2, t3, t4, t5)
        built.clear()
        for step in plan:
            level, k = divmod(step, 10)
            if level == 9:
                works[k]()
            else:
                tasks[level](k)
        for k in range(subs):
            arrived(zbox, k, plane, b1)
        for k in range(subs):
            left(sum1, k, n * cb, r2)
            left(sum2, k, cb, r3)
            left(in3, k, cb, b3)
            left(zz1, k, n * cb, b2)
            left(box, k, plane, b1)

    def tile_pass(tiles_ref, from_row, first_row, source_ref, seg_ref):
        group = min(32, slots)

        def step(number, total):
            for inner in range(group):
                t = number * group + inner
                lhs = source_ref[find(from_row, source_ref.shape[0] - 1, t)]
                out = jnp.dot(
                    jnp.concatenate([lhs, lhs], axis=1), tiles_ref[t],
                    preferred_element_type=f32,
                )
                fresh = tab[first_row, t] == 1
                total = jnp.where(fresh, 0.0, total) + (out[:targets] + out[targets:])
                seg_ref[t] = total
            return total

        lax.fori_loop(0, slots // group, step, jnp.zeros((targets, blk), f32))

    def forward():
        tile_pass(fwd_ref, FWD_FROM, FWD_FIRST, pb_ref, wseg)

    def backward():
        tile_pass(bwd_ref, BWD_FROM, BWD_FIRST, wb_ref, qseg)

    def loop(count, body, init=0, unroll=4):
        return lax.fori_loop(0, count, body, init, unroll=unroll)

    zero = jnp.zeros((targets, blk), f32)
    wseg[slots] = zero
    qseg[slots] = zero

    loads[0].wait()
    loads[1].wait()
    loads[2].start()
    loads[3].start()
    publish(0).wait()
    pl.semaphore_wait(barrier, len(greeted))
    for p in range(KINDS):
        for dc, da in line:
            remote(
                tags_ref.at[p, pl.ds(dc * n + da, 1)],
                tagin.at[p, pl.ds(dc * n + back(da), 1)],
                tag_s.at[p], tag_r.at[p], device(ORDERS[p][0], da, dc),
            ).start()

    lane = lax.broadcasted_iota(jnp.int32, (PIECE, blk), 1)

    def count_send(stage):
        ring_sends(stage, ORDERS[0][stage + 1], False, 1, cin, cin, cnt_s, cnt_r)

    def count_total(stage, size):
        arrived(cin, stage, 1, (cnt_s, cnt_r))
        left(cin, stage, 1, (cnt_s, cnt_r))
        total = cin[stage, 0]
        for s in range(1, n):
            total = total + pltpu.roll(cin[stage, s], blk - back(s) * size, 1)
        return total

    def learn():
        sort_tiles(1, 2, row_blocks, FWD_TILE, ROW_LAST)
        sort_tiles(2, 1, local_cols, BWD_TILE, COL_LAST)
        publish(1).start()
        for p in range(KINDS):
            tagin[p, 0] = tags_ref[p, 0]
            arrived(tagin, p, 1, tagged)
            left(tagin, p, 1, tagged)

            def expand(s, carry):
                row = tagin[p, s]
                for i in range(plane):
                    tagx[p, i * groups + s] = jnp.broadcast_to(row[:, i : i + 1], (PIECE, blk))
                return carry

            loop(groups, expand, unroll=1)

        def census(i, held):
            total = [jnp.zeros((PIECE, blk), f32)] * cb
            for s in range(groups):
                tag = tagx[0, i * groups + s]
                total = [t + jnp.where(tag == b, 1.0, 0.0) for b, t in enumerate(total)]
            for b in range(cb):
                held = jnp.where(lane == i * cb + b, total[b], held)
            return held

        cin[0, 0] = loop(plane, census, jnp.zeros((PIECE, blk), f32), unroll=1)
        count_send(0)

    def ready():
        def opening(c, carry):
            pb_ref[c] = split(x_ref[c])
            return carry

        loop(local_cols, opening)
        loads[2].wait()
        publish(1).wait()

        def convert(t, carry):
            fwd_ref[t] = split(tile_ref[find(FWD_TILE, slots - 1, t)].T)
            bwd_ref[t] = split(tile_ref[find(BWD_TILE, slots - 1, t)])
            return carry

        loop(slots, convert)
        cin[1, 0] = count_total(0, n * cb)
        count_send(1)

    def towards():
        forward()
        loads[3].wait()

        def against(r, carry):
            wb_ref[r] = split(obs_ref[r] - wseg[find(ROW_LAST, slots, r)])
            return carry

        loop(row_blocks, against)
        total = count_total(1, cb)
        for b in range(cb):
            share = jnp.maximum(total[:, b : b + 1], 1.0)
            share_ref[b] = jnp.broadcast_to(share, (PIECE, blk))

    def basis():
        backward()

        def one(c, carry):
            r_ref[c] = qseg[find(COL_LAST, slots, c)] - COUPLING * x_ref[c]
            return carry

        loop(local_cols, one)

    exchange(FIRST_PLAN, (learn, ready, towards, basis))

    gap_line = ORDERS[0]

    def gap_send(stage):
        if stage == 0:
            for dc, da in line:
                remote(
                    gin.at[0, pl.ds(0, 1)], gin.at[0, pl.ds(dc * n + back(da), 1)],
                    gap_s.at[0], gap_r.at[0], device(gap_line[0], da, dc),
                ).start()
        else:
            ring_sends(stage, gap_line[stage], False, 1, gin, gin, gap_s, gap_r)

    def gap_total(stage):
        count = groups if stage == 0 else n
        part = gin.at[stage, pl.ds(1, count - 1)]
        one = remote(part, part, gap_s.at[stage], gap_r.at[stage], anyone)
        one.wait_recv()
        one.wait_send()
        total = gin[stage, 0]
        for s in range(1, count):
            total = total + gin[stage, s]
        return total

    for outer_step in range(ITERS):
        last = outer_step == ITERS - 1

        def begin(c, carry):
            rr, gap = carry
            z = jnp.concatenate(
                [zbox[k, find(MAIL + order(k), zbox.shape[1] - 1, c)] for k in range(subs)], axis=0
            )
            d = x_ref[c] - z
            u = u_ref[c] + d
            u_ref[c] = u
            zu = z - u
            r = r_ref[c] + COUPLING * zu
            r_ref[c] = r
            p_ref[c] = r
            pb_ref[c] = split(r)
            if last:
                gap = gap + d * d
            else:
                zu_ref[c] = zu
            return rr + r * r, gap

        rr, gap = loop(local_cols, begin, (zero, zero), unroll=2)
        rr = lanes(rr)
        pp = rr
        if last:
            gin[0, 0] = lax.dot_general(
                jnp.ones((PIECE, blk), f32),
                jnp.concatenate([gap, jnp.zeros((blk - targets, blk), f32)], axis=0),
                (((1,), (1,)), ((), ())),
                precision=lax.Precision.HIGHEST, preferred_element_type=f32,
            )
            gap_send(0)

        for step in range(CG_STEPS):
            closing = step == CG_STEPS - 1
            forward()

            def image(i, ww):
                w = wseg[find(ROW_LAST, slots, i)]
                if not (last and closing):
                    wb_ref[i] = split(w)
                return ww + w * w

            ww = lanes(loop(row_blocks, image, zero))
            size = rr / (ww + COUPLING * pp)
            if closing:

                def finish(c, carry):
                    x_ref[c] = x_ref[c] + size * p_ref[c]
                    return carry

                loop(local_cols, finish)
                if last:
                    break
                def rest_of_step():
                    backward()

                    def close(c, carry):
                        q = qseg[find(COL_LAST, slots, c)] + COUPLING * p_ref[c]
                        r_ref[c] = r_ref[c] - size * q - COUPLING * zu_ref[c]
                        return carry

                    loop(local_cols, close)

                exchange(NEXT_PLAN, (rest_of_step,))
                break
            backward()
            if last and step < 2:
                gin[step + 1, 0] = gap_total(step)
                gap_send(step + 1)

            def reduce(c, total):
                q = qseg[find(COL_LAST, slots, c)] + COUPLING * p_ref[c]
                r = r_ref[c] - size * q
                r_ref[c] = r
                return total + r * r

            norm = lanes(loop(local_cols, reduce, zero))
            turn = norm / rr

            def direct(c, total):
                old = p_ref[c]
                x_ref[c] = x_ref[c] + size * old
                p = r_ref[c] + turn * old
                p_ref[c] = p
                pb_ref[c] = split(p)
                return total + p * p

            pp = lanes(loop(local_cols, direct, zero))
            rr = norm
    gap_ref[...] = jnp.sqrt(gap_total(2) / mean_of)


def deliver_kernel(x_ref, u_ref, z_ref, gap_ref, x_hbm, u_hbm, z_hbm, out_ref, sems):
    copies = [
        pltpu.make_async_copy(source, target, sems.at[i])
        for i, (source, target) in enumerate(((x_ref, x_hbm), (u_ref, u_hbm), (z_ref, z_hbm)))
    ]
    for one in copies:
        one.start()
    out_ref[...] = gap_ref[0, : out_ref.shape[0]]
    for one in copies:
        one.wait()


def on_device(
    tile_data, tile_row, tile_col, tile_count, touched, owner_map, observed, start_x, start_u
):
    nd, n = lax.axis_size(AXES[0]), lax.axis_size(AXES[1])
    shards = nd * n
    local_cols = touched.shape[1]
    col_blocks = owner_map.shape[0]
    cb = col_blocks // shards
    row_blocks = observed.shape[0]
    slots, blk, _ = tile_data.shape
    targets = start_x.shape[2]
    subs = targets // PIECE
    plane, groups, ring = n * n, 2 * n, n * cb
    f32, b16, i32 = jnp.float32, jnp.bfloat16, jnp.int32
    shape = jax.ShapeDtypeStruct
    assert nd == 2 * n * n and shards == 128 and subs == len(SUB_ORDER)
    assert max(local_cols, slots, row_blocks) <= blk and targets % PIECE == 0

    def padded(v):
        return jnp.pad(v, ((0, 0), (0, blk - v.shape[1])), constant_values=-1)

    raw = jnp.concatenate(
        [
            padded(touched), padded(tile_row), padded(tile_col),
            jnp.broadcast_to(tile_count[:, None], (1, blk)),
            owner_map.reshape(-1, blk),
        ],
        axis=0,
    )

    x = jnp.swapaxes(start_x, 1, 2)
    u = jnp.swapaxes(start_u, 1, 2)
    obs = jnp.swapaxes(observed, 1, 2)
    vec = (local_cols, targets, blk)
    pieces = lambda *lead: pltpu.VMEM((*lead, PIECE, blk), f32)
    dma = lambda *count: pltpu.SemaphoreType.DMA(count)
    vm = pl.BlockSpec(memory_space=pltpu.VMEM)
    hbm = pl.BlockSpec(memory_space=pltpu.HBM)
    x, u, zown, gap = pl.pallas_call(
        functools.partial(kernel, n, cb, shards * local_cols * blk),
        out_shape=(
            shape(vec, f32), shape(vec, f32), shape((cb, targets, blk), f32),
            shape((PIECE, blk), f32),
        ),
        in_specs=[vm, hbm, hbm, hbm, hbm],
        out_specs=(vm,) * 4,
        scratch_shapes=[
            pltpu.VMEM((2 * PIECE, blk), i32), pltpu.SMEM((2 * PIECE, blk), i32),
            pieces(KINDS, groups),
            pltpu.VMEM((slots, blk, blk), f32),
            pltpu.VMEM((slots, 2 * blk, blk), b16),
            pltpu.VMEM((slots, 2 * blk, blk), b16),
            pltpu.VMEM((local_cols, 2 * targets, blk), b16),
            pltpu.VMEM((row_blocks, 2 * targets, blk), b16),
            pltpu.VMEM((slots + 1, targets, blk), f32),
            pltpu.VMEM((slots + 1, targets, blk), f32),
            pltpu.VMEM(vec, f32), pltpu.VMEM(vec, f32), pltpu.VMEM(vec, f32),
            pieces(subs, shards), pieces(subs, shards),
            pieces(subs, plane * cb), pieces(subs, plane * cb),
            pieces(subs, ring), pieces(subs, ring),
            pieces(subs, ring), pieces(subs, plane * cb),
            pieces(subs, shards),
            pieces(KINDS, groups), pieces(KINDS, shards),
            pieces(cb), pieces(3, groups), pieces(2, n),
            dma(4), dma(2), dma(subs), dma(subs),
            dma(subs), dma(subs), dma(subs), dma(subs),
            dma(subs), dma(subs), dma(subs), dma(subs), dma(subs), dma(subs),
            dma(KINDS), dma(KINDS), dma(3), dma(3), dma(2), dma(2),
        ],
        compiler_params=pltpu.CompilerParams(
            vmem_limit_bytes=VMEM_MIB * MIB, has_side_effects=True, collective_id=0
        ),
        name="admm",
    )(raw, tile_data, obs, x, u)
    x, u, zown, primal_gap = pl.pallas_call(
        deliver_kernel,
        out_shape=(
            shape(vec, f32), shape(vec, f32), shape((cb, targets, blk), f32),
            shape((targets,), f32),
        ),
        in_specs=[vm] * 4,
        out_specs=(hbm, hbm, hbm, vm),
        scratch_shapes=[dma(3)],
        compiler_params=pltpu.CompilerParams(vmem_limit_bytes=MIB),
        name="deliver",
    )(x, u, zown, gap)
    return (jnp.swapaxes(x, 1, 2), jnp.swapaxes(u, 1, 2), jnp.swapaxes(zown, 1, 2), primal_gap)


def solution(mesh):
    both = P(AXES)
    placed = (
        P(AXES, None, None), P(AXES, None), P(AXES, None), both, P(AXES, None), P(),
        P(AXES, None, None), P(AXES, None, None), P(AXES, None, None),
    )
    return jax.shard_map(
        on_device,
        mesh=mesh,
        in_specs=placed,
        out_specs=(P(AXES, None, None), P(AXES, None, None), P(AXES, None, None), P()),
        check_vma=False,
    )
```
